32 devices in a mesh: dp: 2 (over x), tp: 4 (over z), ep: 4 (over y, core).
Axes of the slice: x: 2, y: 2, z: 4, core: 2. Of those that a mesh axis runs over, the one named last changes fastest.
Arguments:
- tokens: bfloat16 [8, 32, 2048], P(('dp', 'ep')), parts along dimension 0
- topk_idx: int32 [8, 32, 8], P(('dp', 'ep')), parts along dimension 0
- ln1_gain: bfloat16 [2048], replicated
- w_qkv: bfloat16 [2048, 16, 3, 128], P(None, 'tp')
- w_out: bfloat16 [2048, 2048], P('tp')
- ln2_gain: bfloat16 [2048], replicated
- w_router: bfloat16 [2048, 64], replicated
- w_gate: bfloat16 [64, 2048, 1024], P('ep', None, 'tp')
- w_up: bfloat16 [64, 2048, 1024], P('ep', None, 'tp')
- w_down: bfloat16 [64, 1024, 2048], P('ep', 'tp')
Outputs:
- output: bfloat16 [8, 32, 2048], P(('dp', 'ep')), parts along dimension 0
There are 2 independent parts. The reference program is written for one: setup_inputs(seed, part) draws one part's arguments, and reference() takes and returns one part's arrays. A program takes and returns all parts, laid end to end along the dimension named above; an argument that names none is the same for every part.
All inputs are finite; a program needn't handle non-finite values.
Results may differ from the reference program's by a relative error of at most 0.00897813.
Values are sent between devices in bfloat16 or wider.
A program may use at most 1 GiB of HBM per device.

```python
import jax
import jax.numpy as jnp
from jax import lax

HIDDEN = 2048
HEADS = 16
KV_HEADS = 16
HEAD_DIM = 128
EXPERTS = 64
TOP_K = 8
FFN = 1024
PROMPT_LEN = 32
PROMPTS_DEV = 1
EP_SIZE = 4

GROUP = HEADS // KV_HEADS
TOKENS_DEV = PROMPTS_DEV * PROMPT_LEN
N_PROMPTS = EP_SIZE * PROMPTS_DEV
SEQ_LEN = EP_SIZE * TOKENS_DEV
CAPACITY = 3 * TOKENS_DEV * TOP_K // (2 * EXPERTS)
LOAD_MAX = EP_SIZE * CAPACITY
ROPE_BASE = 500000.0
CLIP_QKV = 8.0
NORM_EPS = 1e-5


def draw_choices(rand_key):
    mean_load = TOKENS_DEV * TOP_K // EXPERTS
    half_load = mean_load // 2
    key_perm, key_dev, key_rot, key_row = jax.random.split(rand_key, 4)
    expert_order = jax.random.permutation(key_perm, EXPERTS)
    spread = jax.random.randint(key_dev, (EXPERTS // 2,), 0, half_load + 1).at[0].set(half_load)
    expert_loads = jnp.zeros((EXPERTS,), jnp.int32).at[expert_order].set(mean_load + jnp.concatenate([spread, -spread]))
    load_ends = jnp.cumsum(expert_loads)
    tickets = jnp.sum((jnp.arange(TOKENS_DEV * TOP_K)[:, None] >= load_ends[None, :]).astype(jnp.int32), axis=1)
    choice = tickets.reshape(TOP_K, TOKENS_DEV).T
    row_shift = jax.random.randint(key_rot, (TOKENS_DEV, 1), 0, TOP_K)
    col_order = (jnp.arange(TOP_K)[None, :] + row_shift) % TOP_K
    choice = jnp.take_along_axis(choice, col_order, axis=1)
    return choice[jax.random.permutation(key_row, TOKENS_DEV)].astype(jnp.int32)


def setup_inputs(seed: int = 0, part: int = 0) -> dict:
    shared_keys = jax.random.split(jax.random.key(seed), 10)
    local_keys = jax.random.split(jax.random.fold_in(jax.random.key(seed + 1), part), EP_SIZE + 1)
    tokens = jax.random.normal(local_keys[0], (N_PROMPTS, PROMPT_LEN, HIDDEN), jnp.float32)
    topk_idx = jax.vmap(draw_choices)(local_keys[1:]).reshape(N_PROMPTS, PROMPT_LEN, TOP_K)
    qkv_scale = jax.random.uniform(shared_keys[0], (KV_HEADS, GROUP + 2, HEAD_DIM), jnp.float32, 1.0, 5.0)
    w_qkv = jax.random.normal(shared_keys[1], (HIDDEN, KV_HEADS, GROUP + 2, HEAD_DIM), jnp.float32) * qkv_scale * HIDDEN ** -0.5
    w_out = jax.random.normal(shared_keys[2], (HEADS * HEAD_DIM, HIDDEN), jnp.float32) * 0.5 * (HEADS * HEAD_DIM) ** -0.5
    ln1_gain = 1.0 + 0.25 * jax.random.normal(shared_keys[3], (HIDDEN,), jnp.float32)
    ln2_gain = 1.0 + 0.25 * jax.random.normal(shared_keys[4], (HIDDEN,), jnp.float32)
    w_router = jax.random.normal(shared_keys[5], (HIDDEN, EXPERTS), jnp.float32) * HIDDEN ** -0.5
    w_gate = jax.random.normal(shared_keys[6], (EXPERTS, HIDDEN, FFN), jnp.float32) * HIDDEN ** -0.5
    w_up = jax.random.normal(shared_keys[7], (EXPERTS, HIDDEN, FFN), jnp.float32) * HIDDEN ** -0.5
    w_down = jax.random.normal(shared_keys[8], (EXPERTS, FFN, HIDDEN), jnp.float32) * 2.0 * FFN ** -0.5
    return {
        "tokens": tokens.astype(jnp.bfloat16),
        "topk_idx": topk_idx,
        "ln1_gain": ln1_gain.astype(jnp.bfloat16),
        "w_qkv": w_qkv.astype(jnp.bfloat16),
        "w_out": w_out.astype(jnp.bfloat16),
        "ln2_gain": ln2_gain.astype(jnp.bfloat16),
        "w_router": w_router.astype(jnp.bfloat16),
        "w_gate": w_gate.astype(jnp.bfloat16),
        "w_up": w_up.astype(jnp.bfloat16),
        "w_down": w_down.astype(jnp.bfloat16),
    }


def layer_norm(values_in, gain_vec):
    mean_val = jnp.mean(values_in, axis=-1, keepdims=True)
    centered = values_in - mean_val
    var_val = jnp.mean(centered * centered, axis=-1, keepdims=True)
    return (centered * lax.rsqrt(var_val + NORM_EPS) * gain_vec.astype(jnp.float32)).astype(jnp.bfloat16)


def apply_rope(values_in, cos_tab, sin_tab):
    half_dim = values_in.shape[-1] // 2
    first_half = values_in[..., :half_dim]
    second_half = values_in[..., half_dim:]
    return jnp.concatenate([first_half * cos_tab - second_half * sin_tab, second_half * cos_tab + first_half * sin_tab], axis=-1)


def reference(tokens, topk_idx, ln1_gain, w_qkv, w_out, ln2_gain, w_router, w_gate, w_up, w_down):
    inv_freq = ROPE_BASE ** (-jnp.arange(HEAD_DIM // 2, dtype=jnp.float32) * (2.0 / HEAD_DIM))
    angles = jnp.arange(PROMPT_LEN, dtype=jnp.float32)[:, None] * inv_freq[None, :]
    cos_tab = jnp.cos(angles)
    sin_tab = jnp.sin(angles)
    causal = jnp.arange(PROMPT_LEN)[:, None] >= jnp.arange(PROMPT_LEN)[None, :]

    def one_prompt(prompt):
        normed = layer_norm(prompt.astype(jnp.float32), ln1_gain)
        qkv_all = jnp.dot(normed, w_qkv.reshape(HIDDEN, KV_HEADS * (GROUP + 2) * HEAD_DIM), preferred_element_type=jnp.float32).astype(jnp.bfloat16)
        qkv_all = jnp.clip(qkv_all, -CLIP_QKV, CLIP_QKV).reshape(PROMPT_LEN, KV_HEADS, GROUP + 2, HEAD_DIM)
        query_rot = apply_rope(qkv_all[:, :, :GROUP].astype(jnp.float32), cos_tab[:, None, None, :], sin_tab[:, None, None, :]).astype(jnp.bfloat16)
        key_rot = apply_rope(qkv_all[:, :, GROUP].astype(jnp.float32), cos_tab[:, None, :], sin_tab[:, None, :]).astype(jnp.bfloat16)
        value_rows = qkv_all[:, :, GROUP + 1]
        scores = jnp.einsum("qgrd,kgd->grqk", query_rot.astype(jnp.float32), key_rot.astype(jnp.float32)) * HEAD_DIM ** -0.5
        scores = jnp.where(causal, scores, -1e30)
        probs = jax.nn.softmax(scores, axis=-1).astype(jnp.bfloat16)
        mixed = jnp.einsum("grqk,kgd->qgrd", probs.astype(jnp.float32), value_rows.astype(jnp.float32)).astype(jnp.bfloat16)
        attn_out = jnp.dot(mixed.reshape(PROMPT_LEN, HEADS * HEAD_DIM), w_out, preferred_element_type=jnp.float32)
        return prompt.astype(jnp.float32) + attn_out

    resid = lax.map(one_prompt, tokens).reshape(SEQ_LEN, HIDDEN)
    normed = layer_norm(resid, ln2_gain)
    choice = topk_idx.reshape(SEQ_LEN, TOP_K)
    probs_all = jax.nn.softmax(jnp.dot(normed, w_router, preferred_element_type=jnp.float32), axis=-1)
    picked = jnp.take_along_axis(probs_all, choice, axis=1)
    weights = picked / jnp.sum(picked, axis=1, keepdims=True)
    flat_choice = choice.reshape(-1)
    hit_mask = (flat_choice[:, None] == jnp.arange(EXPERTS)[None, :]).astype(jnp.int32)
    slot_rank = jnp.sum((jnp.cumsum(hit_mask, axis=0) - 1) * hit_mask, axis=1)
    slot_ids = flat_choice * LOAD_MAX + slot_rank
    owners = jnp.full((EXPERTS * LOAD_MAX,), SEQ_LEN, jnp.int32).at[slot_ids].set(jnp.arange(SEQ_LEN * TOP_K, dtype=jnp.int32) // TOP_K)
    slot_coef = jnp.zeros((EXPERTS * LOAD_MAX,), jnp.float32).at[slot_ids].set(weights.reshape(-1))

    def expert_step(acc_sum, pack_in):
        gate_w, up_w, down_w, row_ids, row_coef = pack_in
        rows_in = jnp.take(normed, row_ids, axis=0, mode="fill", fill_value=0)
        gate_act = jnp.dot(rows_in, gate_w, preferred_element_type=jnp.float32)
        up_act = jnp.dot(rows_in, up_w, preferred_element_type=jnp.float32)
        hidden_act = (jax.nn.silu(gate_act) * up_act).astype(jnp.bfloat16)
        expert_rows = jnp.dot(hidden_act, down_w, preferred_element_type=jnp.float32)
        return acc_sum.at[row_ids].add(expert_rows * row_coef[:, None], mode="drop"), None

    moe_sum = lax.scan(expert_step, jnp.zeros((SEQ_LEN, HIDDEN), jnp.float32), (w_gate, w_up, w_down, owners.reshape(EXPERTS, LOAD_MAX), slot_coef.reshape(EXPERTS, LOAD_MAX)))[0]
    return (resid + moe_sum).astype(jnp.bfloat16).reshape(N_PROMPTS, PROMPT_LEN, HIDDEN)
```

```python
import functools

import jax
import jax.numpy as jnp
import numpy as np
from jax import lax
from jax.experimental import pallas as pl
from jax.experimental.pallas import tpu as pltpu
from jax.sharding import PartitionSpec as P

ROPE_BASE = 500000.0
CLIP_QKV = 8.0
NORM_EPS = 1e-5
F32 = jnp.float32
BF16 = jnp.bfloat16
MESH = pl.DeviceIdType.MESH

LANES = 128
KTILE = 256
QKV_CHUNKS = 4
OUT_BLOCKS = 4


def normalize(rows, gain_ref):
    mean_val = jnp.mean(rows, axis=-1, keepdims=True)
    centered = rows - mean_val
    var_val = jnp.mean(centered * centered, axis=-1, keepdims=True)
    inv_std = lax.rsqrt(var_val + NORM_EPS)
    for blk in range(rows.shape[-1] // LANES):
        cols = slice(blk * LANES, (blk + 1) * LANES)
        gain_row = gain_ref[blk : blk + 1, :].astype(F32)
        yield blk, (centered[:, cols] * inv_std * gain_row).astype(BF16)


def layer_kernel(
    x_ref, x3_ref, topk_ref, gain1_ref, gain2_ref, cos_ref, sin_ref,
    wqkv_hbm, wout_hbm, wr_hbm, wg_hbm, wu_hbm, wd_hbm,
    out_ref,
    wqkv, wout, wr, wg, wu, wd, lhs, part_f32, part_send, part_recv, g_all, x1_own, topk_all,
    coef, acc, c1_send, c1_recv, c2_send, c2_recv, c3_send, c3_recv, y_all,
    wq_sem, wm_sem, wg_sem, wu_sem, wd_sem,
    rs_ss, rs_rs, g_ss, g_rs, tk_ss, tk_rs, c1_ss, c1_rs, c2_ss, c2_rs, c3_ss, c3_rs, y_ss, y_rs,
):
    z = lax.axis_index("tp")
    ep = lax.axis_index("ep")
    core = lax.rem(ep, 2)
    ypos = ep // 2
    partner = ep + 1 - 2 * core
    across = lax.rem(ep + 2, 4)
    diagonal = lax.rem(partner + 2, 4)
    z_order = [lax.rem(z + d, 4) for d in (2, 1, 3)]
    n_loc = wg.shape[0]
    hidden = x_ref.shape[1]
    rows_dev = x_ref.shape[0]
    heads = wqkv.shape[2]

    barrier = pltpu.get_barrier_semaphore()
    for zp in z_order:
        pl.semaphore_signal(barrier, inc=1, device_id={"tp": zp}, device_id_type=MESH)
    for other in (partner, across, diagonal):
        pl.semaphore_signal(barrier, inc=1, device_id={"ep": other}, device_id_type=MESH)

    chunk_rows = hidden // QKV_CHUNKS
    loads_qkv = []
    for ch in range(QKV_CHUNKS):
        for kind in range(3):
            rows = pl.ds(ch * chunk_rows, chunk_rows)
            loads_qkv.append(pltpu.make_async_copy(wqkv_hbm.at[rows, kind], wqkv.at[kind, rows], wq_sem.at[ch * 3 + kind]))
    for copy in loads_qkv:
        copy.start()
    load_wout = pltpu.make_async_copy(wout_hbm, wout, wm_sem.at[0])
    load_wout.start()
    load_wr = pltpu.make_async_copy(wr_hbm, wr, wm_sem.at[1])
    load_wr.start()

    def load_gate(e):
        return pltpu.make_async_copy(wg_hbm.at[e], wg.at[e], wg_sem.at[e])

    def load_up(e):
        return pltpu.make_async_copy(wu_hbm.at[e], wu.at[e], wu_sem.at[e])

    def load_down(e):
        return pltpu.make_async_copy(wd_hbm.at[e], wd.at[e], wd_sem.at[e])

    for e in range(n_loc):
        load_gate(e).start()
        load_up(e).start()
    for e in range(n_loc):
        load_down(e).start()

    tokens_f32 = x_ref[...].astype(F32)
    spread_row = lax.broadcasted_iota(jnp.int32, (LANES, heads * LANES), 0)
    spread_col = lax.broadcasted_iota(jnp.int32, (LANES, heads * LANES), 1)
    spread = (lax.shift_right_logical(spread_col, 2) == spread_row).astype(BF16)
    lane_head = lax.rem(lax.broadcasted_iota(jnp.int32, (rows_dev, heads * LANES), 1), heads)
    for blk, normed in normalize(tokens_f32, gain1_ref):
        wide = jnp.dot(normed, spread, preferred_element_type=F32)
        for h in range(heads):
            picked = jnp.where(lane_head == h, wide, 0.0).astype(BF16)
            for part in range(2):
                lhs[2 * blk + part, h * rows_dev : (h + 1) * rows_dev, :] = picked[:, part * KTILE : (part + 1) * KTILE]

    wqkv_rows = wqkv.reshape(3, hidden * heads, LANES)
    tiles = hidden * heads // KTILE // QKV_CHUNKS
    qkv = [None, None, None]
    for ch in range(QKV_CHUNKS):
        for kind in range(3):
            loads_qkv[ch * 3 + kind].wait()
        for kt in range(ch * tiles, (ch + 1) * tiles):
            left = lhs[kt]
            for kind in range(3):
                term = jnp.dot(left, wqkv_rows[kind, kt * KTILE : (kt + 1) * KTILE, :], preferred_element_type=F32)
                qkv[kind] = term if qkv[kind] is None else qkv[kind] + term
    qkv = [jnp.clip(v.astype(BF16), -CLIP_QKV, CLIP_QKV) for v in qkv]

    cos_tab = jnp.concatenate([cos_ref[...]] * heads, axis=0)
    sin_tab = jnp.concatenate([sin_ref[...]] * heads, axis=0)

    def rope(v):
        wide = v.astype(F32)
        return (wide * cos_tab + pltpu.roll(wide, LANES // 2, 1) * sin_tab).astype(BF16)

    scores = lax.dot_general(rope(qkv[0]), rope(qkv[1]), (((1,), (1,)), ((), ())), preferred_element_type=F32)
    scores = scores * LANES ** -0.5
    q_pos = lax.broadcasted_iota(jnp.int32, scores.shape, 0)
    k_pos = lax.broadcasted_iota(jnp.int32, scores.shape, 1)
    same_head = lax.shift_right_logical(q_pos, 5) == lax.shift_right_logical(k_pos, 5)
    scores = jnp.where(same_head & (q_pos >= k_pos), scores, -1e30)
    scores = jnp.exp(scores - jnp.max(scores, axis=-1, keepdims=True))
    probs = (scores / jnp.sum(scores, axis=-1, keepdims=True)).astype(BF16)
    mixed = jnp.dot(probs, qkv[2], preferred_element_type=F32).astype(BF16)
    mixed = jnp.concatenate([mixed[h * rows_dev : (h + 1) * rows_dev] for h in range(heads)], axis=1)
    load_wout.wait()
    attn = jnp.dot(mixed, wout[...], preferred_element_type=F32)
    for zp in range(4):
        piece = attn[zp * 8 : (zp + 1) * 8]
        part_f32[zp] = piece
        part_send[zp] = piece.astype(BF16)

    pl.semaphore_wait(barrier, 6)

    def rs_copy(d, zp):
        return pltpu.make_async_remote_copy(part_send.at[zp], part_recv.at[z], rs_ss.at[d], rs_rs.at[z], device_id={"tp": zp}, device_id_type=MESH)

    rs_sends = [rs_copy(d, zp) for d, zp in enumerate(z_order)]
    for copy in rs_sends:
        copy.start()
    tk_sends = []
    for d, other in enumerate((partner, across, diagonal)):
        copy = pltpu.make_async_remote_copy(topk_ref, topk_all.at[ep], tk_ss.at[d], tk_rs.at[ep], device_id={"ep": other}, device_id_type=MESH)
        copy.start()
        tk_sends.append(copy)
    topk_all[ep] = topk_ref[...]

    x1 = x3_ref[z].astype(F32)
    total = part_f32[z]
    for zp in (z_order[1], z_order[2], z_order[0]):
        pltpu.make_async_remote_copy(part_send.at[zp], part_recv.at[zp], rs_ss.at[0], rs_rs.at[zp], device_id={"tp": zp}, device_id_type=MESH).wait_recv()
        total = total + part_recv[zp].astype(F32)
    x1 = x1 + total
    x1_own[...] = x1
    for blk, normed in normalize(x1, gain2_ref):
        g_all[ep * 4 + z, :, blk * LANES : (blk + 1) * LANES] = normed

    g_sends = []

    def send_piece(e, zp, **device):
        piece = e * 4 + zp
        copy = pltpu.make_async_remote_copy(g_all.at[piece], g_all.at[piece], g_ss.at[len(g_sends)], g_rs.at[piece], device_id=device, device_id_type=MESH)
        copy.start()
        g_sends.append(copy)

    def wait_piece(e, zp):
        piece = e * 4 + zp
        pltpu.make_async_remote_copy(g_all.at[piece], g_all.at[piece], g_ss.at[0], g_rs.at[piece], device_id={"tp": z_order[0]}, device_id_type=MESH).wait_recv()

    for zp in z_order:
        send_piece(ep, z, tp=zp)
    send_piece(ep, z, ep=across)
    send_piece(ep, z, ep=partner)
    near = [z, z_order[1], z_order[2], z_order[0]]
    for i, zp in enumerate(near):
        if i > 0:
            wait_piece(ep, zp)
            send_piece(ep, zp, ep=across)
            send_piece(ep, zp, ep=partner)
    for zp in near:
        wait_piece(across, zp)
        send_piece(across, zp, ep=partner)
    for e in (partner, diagonal):
        for zp in near:
            wait_piece(e, zp)
    k_tiles = hidden // KTILE
    for kt in range(k_tiles):
        lhs[n_loc + kt] = jnp.concatenate([g_all[p, :, kt * KTILE : (kt + 1) * KTILE] for p in range(16)], axis=0)

    def over_g(dot_tile):
        total = dot_tile(lhs[n_loc], slice(0, KTILE))
        for kt in range(1, k_tiles):
            total = total + dot_tile(lhs[n_loc + kt], slice(kt * KTILE, (kt + 1) * KTILE))
        return total


    for other in (partner, across, diagonal):
        pltpu.make_async_remote_copy(topk_ref, topk_all.at[other], tk_ss.at[0], tk_rs.at[other], device_id={"ep": other}, device_id_type=MESH).wait_recv()
    load_wr.wait()
    logits = over_g(lambda g, ks: lax.dot_general(wr[:, ks], g, (((1,), (1,)), ((), ())), preferred_element_type=F32))
    logits = jnp.exp(logits - jnp.max(logits, axis=0, keepdims=True))
    route = logits / jnp.sum(logits, axis=0, keepdims=True)
    choice = jnp.concatenate([topk_all[e] for e in range(4)], axis=1)
    expert_id = lax.broadcasted_iota(jnp.int32, route.shape, 0)
    chosen = expert_id == choice[0:1, :]
    for k in range(1, choice.shape[0]):
        chosen = chosen | (expert_id == choice[k : k + 1, :])
    route = jnp.where(chosen, route, 0.0)
    route = route / jnp.sum(route, axis=0, keepdims=True)
    coef[0 : route.shape[0], :] = route
    local = coef[pl.ds(pl.multiple_of(ep * n_loc, 8), n_loc), :]
    local = jnp.concatenate([local, jnp.zeros((LANES - n_loc, LANES), F32)], axis=0)
    coef[...] = local.T

    def up_step(e, carry):
        load_gate(e).wait()
        load_up(e).wait()
        gate_act = over_g(lambda g, ks: jnp.dot(g, wg[e, ks, :], preferred_element_type=F32))
        up_act = over_g(lambda g, ks: jnp.dot(g, wu[e, ks, :], preferred_element_type=F32))
        lhs[e] = (gate_act * jax.nn.sigmoid(gate_act) * up_act).astype(BF16)
        return carry

    lax.fori_loop(0, n_loc, up_step, 0, unroll=2)
    for e in range(n_loc):
        load_down(e).wait()

    width = hidden // OUT_BLOCKS

    def down_block(nb):
        for half in range(width // KTILE):
            cols = slice(nb * width + half * KTILE, nb * width + (half + 1) * KTILE)
            total = None
            for e in range(n_loc):
                term = jnp.dot(lhs[e], wd[e, :, cols], preferred_element_type=F32) * coef[:, e : e + 1]
                total = term if total is None else total + term
            for e in range(4):
                acc[nb, e, :, half * KTILE : (half + 1) * KTILE] = total[e * rows_dev : (e + 1) * rows_dev]

    def c1_copy(nb):
        return pltpu.make_async_remote_copy(c1_send.at[nb], c1_recv.at[nb], c1_ss.at[nb], c1_rs.at[nb], device_id={"ep": partner}, device_id_type=MESH)

    def c2_copy(nb):
        return pltpu.make_async_remote_copy(c2_send.at[nb], c2_recv.at[nb], c2_ss.at[nb], c2_rs.at[nb], device_id={"ep": across}, device_id_type=MESH)

    def c3_copy(nb, d, zp):
        return pltpu.make_async_remote_copy(c3_send.at[nb, zp], c3_recv.at[nb, z], c3_ss.at[nb * 3 + d], c3_rs.at[nb * 4 + z], device_id={"tp": zp}, device_id_type=MESH)

    def y_copy(nb, d, zp):
        return pltpu.make_async_remote_copy(y_all.at[nb, z], y_all.at[nb, z], y_ss.at[nb * 3 + d], y_rs.at[nb * 4 + z], device_id={"tp": zp}, device_id_type=MESH)

    def stage1(nb):
        for yp in range(2):
            c1_send[nb, yp] = acc[nb, 2 * yp + 1 - core].astype(BF16)
        c1_copy(nb).start()

    def stage2(nb):
        c1_copy(nb).wait_recv()
        c2_send[nb] = (acc[nb, 2 * (1 - ypos) + core] + c1_recv[nb, 1 - ypos].astype(F32)).astype(BF16)
        c2_copy(nb).start()

    def stage3(nb):
        c2_copy(nb).wait_recv()
        total = acc[nb, ep] + c1_recv[nb, ypos].astype(F32) + c2_recv[nb].astype(F32)
        for zp in range(4):
            part_f32[zp, :, nb * width : (nb + 1) * width] = total[zp * 8 : (zp + 1) * 8]
            c3_send[nb, zp] = total[zp * 8 : (zp + 1) * 8].astype(BF16)
        for d, zp in enumerate(z_order):
            c3_copy(nb, d, zp).start()

    def stage4(nb):
        cols = slice(nb * width, (nb + 1) * width)
        total = part_f32[z, :, cols]
        for zp in (z_order[1], z_order[2], z_order[0]):
            pltpu.make_async_remote_copy(c3_send.at[nb, zp], c3_recv.at[nb, zp], c3_ss.at[nb * 3], c3_rs.at[nb * 4 + zp], device_id={"tp": zp}, device_id_type=MESH).wait_recv()
            total = total + c3_recv[nb, zp].astype(F32)
        y_all[nb, z] = (x1_own[:, cols] + total).astype(BF16)
        for d, zp in enumerate(z_order):
            y_copy(nb, d, zp).start()

    def stage5(nb):
        for zp in (z_order[1], z_order[2], z_order[0]):
            pltpu.make_async_remote_copy(y_all.at[nb, zp], y_all.at[nb, zp], y_ss.at[nb * 3], y_rs.at[nb * 4 + zp], device_id={"tp": zp}, device_id_type=MESH).wait_recv()
        for zp in range(4):
            out_ref[zp, :, nb * width : (nb + 1) * width] = y_all[nb, zp]

    stages = [stage2, stage3, stage4, stage5]
    for step in range(OUT_BLOCKS + len(stages)):
        if step < OUT_BLOCKS:
            down_block(step)
            stage1(step)
        for lag, stage in enumerate(stages):
            nb = step - 1 - lag
            if 0 <= nb < OUT_BLOCKS:
                stage(nb)

    for copy in rs_sends + tk_sends + g_sends:
        copy.wait_send()
    for nb in range(OUT_BLOCKS):
        c1_copy(nb).wait_send()
        c2_copy(nb).wait_send()
        for d, zp in enumerate(z_order):
            c3_copy(nb, d, zp).wait_send()
            y_copy(nb, d, zp).wait_send()


def solution(mesh):
    def device_step(tokens, topk_idx, ln1_gain, w_qkv, w_out, ln2_gain, w_router, w_gate, w_up, w_down):
        rows_dev = tokens.shape[0] * tokens.shape[1]
        length, hidden = tokens.shape[1:]
        n_exp = w_router.shape[1]
        n_loc, _, ffn = w_gate.shape
        top_k = topk_idx.shape[-1]
        heads, head_dim = w_qkv.shape[1], w_qkv.shape[3]
        width = hidden // OUT_BLOCKS
        inv_freq = ROPE_BASE ** (-np.arange(head_dim // 2, dtype=np.float32) * np.float32(2.0 / head_dim))
        angles = np.arange(length, dtype=np.float32)[:, None] * inv_freq[None, :].astype(np.float32)
        cos_tab = np.concatenate([np.cos(angles)] * 2, axis=1).astype(np.float32)
        sin_tab = np.concatenate([-np.sin(angles), np.sin(angles)], axis=1).astype(np.float32)
        vmem = pl.BlockSpec(memory_space=pltpu.VMEM)
        hbm = pl.BlockSpec(memory_space=pl.ANY)
        dma = pltpu.SemaphoreType.DMA
        nb = OUT_BLOCKS
        y = pl.pallas_call(
            layer_kernel,
            name="moe_layer",
            out_shape=jax.ShapeDtypeStruct((4, 8, hidden), BF16),
            in_specs=[vmem] * 7 + [hbm] * 6,
            out_specs=vmem,
            scratch_shapes=[
                pltpu.VMEM((3, hidden, heads, head_dim), BF16),
                pltpu.VMEM((heads * head_dim, hidden), BF16),
                pltpu.VMEM((n_exp, hidden), BF16),
                pltpu.VMEM((n_loc, hidden, ffn), BF16),
                pltpu.VMEM((n_loc, hidden, ffn), BF16),
                pltpu.VMEM((n_loc, ffn, hidden), BF16),
                pltpu.VMEM((hidden * heads // KTILE, heads * rows_dev, KTILE), BF16),
                pltpu.VMEM((4, 8, hidden), F32),
                pltpu.VMEM((4, 8, hidden), BF16),
                pltpu.VMEM((4, 8, hidden), BF16),
                pltpu.VMEM((16, 8, hidden), BF16),
                pltpu.VMEM((8, hidden), F32),
                pltpu.VMEM((4, top_k, rows_dev), jnp.int32),
                pltpu.VMEM((LANES, LANES), F32),
                pltpu.VMEM((nb, 4, rows_dev, width), F32),
                pltpu.VMEM((nb, 2, rows_dev, width), BF16),
                pltpu.VMEM((nb, 2, rows_dev, width), BF16),
                pltpu.VMEM((nb, rows_dev, width), BF16),
                pltpu.VMEM((nb, rows_dev, width), BF16),
                pltpu.VMEM((nb, 4, 8, width), BF16),
                pltpu.VMEM((nb, 4, 8, width), BF16),
                pltpu.VMEM((nb, 4, 8, width), BF16),
                dma((QKV_CHUNKS * 3,)), dma((2,)), dma((n_loc,)), dma((n_loc,)), dma((n_loc,)),
                dma((3,)), dma((4,)), dma((15,)), dma((16,)), dma((3,)), dma((4,)),
                dma((nb,)), dma((nb,)), dma((nb,)), dma((nb,)),
                dma((3 * nb,)), dma((4 * nb,)), dma((3 * nb,)), dma((4 * nb,)),
            ],
            compiler_params=pltpu.CompilerParams(collective_id=0, has_side_effects=True, vmem_limit_bytes=67043328),
        )(
            tokens.reshape(rows_dev, hidden),
            tokens.reshape(4, 8, hidden),
            topk_idx.reshape(rows_dev, top_k).T,
            ln1_gain.reshape(hidden // LANES, LANES),
            ln2_gain.reshape(hidden // LANES, LANES),
            jnp.asarray(cos_tab),
            jnp.asarray(sin_tab),
            jnp.transpose(w_qkv, (0, 2, 1, 3)),
            w_out,
            w_router.T,
            w_gate,
            w_up,
            w_down,
        )
        return y.reshape(tokens.shape)

    tok_spec = P(("dp", "ep"), None, None)
    in_specs = (tok_spec, tok_spec, P(None), P(None, "tp", None, None), P("tp", None), P(None), P(None, None), P("ep", None, "tp"), P("ep", None, "tp"), P("ep", "tp", None))
    return jax.shard_map(device_step, mesh=mesh, in_specs=in_specs, out_specs=tok_spec, check_vma=False)
```
